256 devices in a mesh: bank: 64 (over z, y, core), zero: 4 (over x).
Axes of the slice: x: 4, y: 4, z: 8, core: 2. Of those that a mesh axis runs over, the one named last changes fastest.
Arguments:
- train_down: float32 [128, 768, 2048], P('bank', None, 'zero'), may hold values from -0.3125 to 0.3125
- other_down: float32 [128, 768, 2048], P('bank', None, 'zero'), may hold values from -0.21875 to 0.21875
- router_weight: float32 [2048, 128], P('zero', 'bank'), may hold values from -0.125 to 0.125
- router_gain: float32 [2048], P('zero'), may hold values from 0.25 to 1.75
Outputs:
- ready_down: bfloat16 [128, 768, 2048], P('bank')
- scale_down: float32 [128, 768], P('bank')
- serve_router: bfloat16 [2048, 128], replicated
- latest_down: float32 [128, 768, 2048], P('bank', None, 'zero')
The draws below stay inside these ranges and needn't reach their ends.
All inputs are finite; a program needn't handle non-finite values. Where the reference program divides by a largest or mean magnitude, that divisor is 1e-20 or more.
Results may differ from the reference program's by a relative error of at most 0.001.
Values may be sent and summed in bfloat16 or wider, within the bound.
A program may use at most 128 MiB of HBM per device.

```python
import jax
import jax.numpy as jnp

EXPERTS = 128
D_MODEL = 2048
D_EXPERT = 768


def spiked(drawn, rng, source, target, shards_of, factor):
    def block_of(dim):
        return (jnp.arange(drawn.shape[dim]) // (drawn.shape[dim] // shards_of)).reshape((-1,) + (1,) * (drawn.ndim - 1 - dim))

    first = jax.random.permutation(rng, shards_of)[block_of(target)]
    second = (block_of(target) + shards_of // 2) % shards_of
    return jnp.where((block_of(source) == first) | (block_of(source) == second), factor * drawn, drawn)


def shard_levels(stream_key, extent, pieces, smallest, high):
    gain, own = 1.0, jax.random.fold_in(stream_key, 6)
    for axis_at, blocks in pieces:
        draws = jnp.exp(jax.random.uniform(jax.random.fold_in(own, axis_at), (blocks,), jnp.float32, smallest / len(pieces), high / len(pieces)))
        gain = gain * jnp.repeat(draws, extent[axis_at] // blocks).reshape([-1 if axis == axis_at else 1 for axis in range(len(extent))])
    return gain


def gaussian(key, extent, width, most, pieces=(), kind=jnp.bfloat16):
    entries = width * jax.random.normal(key, extent, jnp.float32)
    if pieces:
        entries = entries * shard_levels(key, extent, pieces, -0.22, 0.18)
    return jnp.clip(entries, -most, most).astype(kind)


def noise_with(own_key, extent, spread, bound, shards, heavy, held_as=jnp.bfloat16):
    entries = spread * jax.random.normal(own_key, extent, jnp.float32)
    if shards:
        entries = entries * shard_levels(own_key, extent, shards, -0.22, 0.18)
    return jnp.clip(spiked(entries, jax.random.fold_in(own_key, 3), *heavy), -bound, bound).astype(held_as)


def setup_inputs(seed: int = 0) -> dict:
    arg_keys = jax.random.split(jax.random.key(seed), 5)
    train_down = noise_with(arg_keys[0], (EXPERTS, D_EXPERT, D_MODEL), D_EXPERT ** -0.5, 0.3125, ((0, 64), (2, 4)), (2, 1, 4, 2.0), jnp.float32)
    other_down = gaussian(arg_keys[1], (EXPERTS, D_EXPERT, D_MODEL), D_EXPERT ** -0.5, 0.21875, ((0, 64), (2, 4)), jnp.float32)
    router_weight = gaussian(arg_keys[2], (D_MODEL, EXPERTS), D_MODEL ** -0.5, 0.125, ((0, 4), (1, 64)), jnp.float32)
    router_gain = jnp.clip(1.0 + 0.15 * jax.random.normal(arg_keys[3], (D_MODEL,), jnp.float32), 0.25, 1.75)
    return {"train_down": train_down, "other_down": other_down, "router_weight": router_weight, "router_gain": router_gain}


def reference(train_down, other_down, router_weight, router_gain):
    latest_down = 0.5 * other_down + 0.5 * train_down
    scale_down = jnp.sum(jnp.abs(latest_down), axis=2) / D_MODEL
    ready_down = (latest_down / jnp.expand_dims(scale_down, 2)).astype(jnp.bfloat16)
    serve_router = (router_weight * router_gain[:, None]).astype(jnp.bfloat16)
    return ready_down, scale_down, serve_router, latest_down
```

```python
import functools

import jax
import jax.numpy as jnp
from jax import lax
from jax.experimental import pallas as pl
from jax.experimental.pallas import tpu as pltpu
from jax.sharding import PartitionSpec as P

MESH = pl.DeviceIdType.MESH
D_MODEL = 2048
ROWS = 1536
PART = 512
BLOCK = 128
BLOCKS = ROWS // BLOCK
CHUNK = 256
CHUNKS = ROWS // CHUNK
HALF = CHUNKS // 2
NZ, NY, NC, NX = 8, 4, 2, 4


def kernel(
    train, other, weight, gain,
    ready, scale, router, latest,
    train_v, other_v, weight_v, gain_v, sums, rows_r, wide_r,
    in_sem, small_sem, sum_s, sum_r, rx_s, rx_r, ry_s, ry_r, rz_s, rz_r, rc_s, rc_r,
    own_s, own_r, far_s, far_r,
):
    me = lax.axis_index("zero")
    bank = lax.axis_index("bank")
    z, y, core = bank // (NY * NC), lax.rem(bank // NC, NY), lax.rem(bank, NC)
    right, left, opposite = (lax.rem(me + k, NX) for k in (1, 3, 2))
    bank_of = lambda z, y, core: (z * NY + y) * NC + core
    z_up, z_down = lax.rem(z + 1, NZ), lax.rem(z + NZ - 1, NZ)
    y_up, y_down = lax.rem(y + 1, NY), lax.rem(y + NY - 1, NY)
    at_y_up, at_y_down = {"bank": bank_of(z, y_up, core)}, {"bank": bank_of(z, y_down, core)}
    at_z_up, at_z_down = {"bank": bank_of(z_up, y, core)}, {"bank": bank_of(z_down, y, core)}
    at_core = {"bank": bank_of(z, y, 1 - core)}
    at_x = [{"zero": right}, {"zero": left}, {"zero": opposite}]

    barrier = pltpu.get_barrier_semaphore()
    for peer in (*at_x, at_y_up, at_y_down, at_z_up, at_z_down, at_core):
        pl.semaphore_signal(barrier, inc=1, device_id=peer, device_id_type=MESH)

    def read(c):
        rows = pl.ds(c * CHUNK, CHUNK)
        return [
            pltpu.make_async_copy(train.at[rows], train_v.at[rows], in_sem.at[0, c]),
            pltpu.make_async_copy(other.at[rows], other_v.at[rows], in_sem.at[1, c]),
        ]

    small = [
        pltpu.make_async_copy(weight, weight_v, small_sem.at[0]),
        pltpu.make_async_copy(gain, gain_v, small_sem.at[1]),
    ]
    reads = [read(c) for c in range(CHUNKS)]
    for copy in (*reads[0], *small, *(r for c in range(1, CHUNKS) for r in reads[c])):
        copy.start()

    def send(src, dst, s, r, to):
        copy = pltpu.make_async_remote_copy(
            src_ref=src, dst_ref=dst, send_sem=s, recv_sem=r, device_id=to, device_id_type=MESH
        )
        copy.start()
        return copy

    def average(c):
        for copy in reads[c]:
            copy.wait()
        for b in range(c * CHUNK // BLOCK, (c + 1) * CHUNK // BLOCK):
            rows = pl.ds(b * BLOCK, BLOCK)
            mixed = 0.5 * other_v[rows, :] + 0.5 * train_v[rows, :]
            latest[rows, :] = mixed
            size = jnp.abs(mixed)
            lanes = sum(size[:, k * 128 : (k + 1) * 128] for k in range(1, PART // 128)) + size[:, :128]
            sums[me, b] = jnp.sum(lanes.T, axis=0, keepdims=True)

    def send_sums(first, last, group):
        blocks = pl.ds(first, last - first)
        return [
            send(sums.at[me, blocks], sums.at[me, blocks], sum_s.at[group, k], sum_r.at[group, k], at_x[k])
            for k in range(3)
        ]

    def narrow(c):
        for b in range(c * CHUNK // BLOCK, (c + 1) * CHUNK // BLOCK):
            rows = pl.ds(b * BLOCK, BLOCK)
            mean = ((sums[0, b] + sums[1, b]) + (sums[2, b] + sums[3, b])) / D_MODEL
            per = BLOCKS // 2
            scale[b // per : b // per + 1, (b % per) * BLOCK : (b % per + 1) * BLOCK] = mean
            factor = jnp.broadcast_to(1.0 / mean, (BLOCK, BLOCK)).T
            for k in range(PART // 128):
                columns = pl.ds(pl.multiple_of(me * PART + k * 128, 128), 128)
                ready[rows, columns] = (latest[rows, k * 128 : (k + 1) * 128] * factor).astype(jnp.bfloat16)

    def block_of(c, x):
        return ready.at[pl.ds(c * CHUNK, CHUNK), pl.ds(pl.multiple_of(x * PART, PART), PART)]

    average(0)
    for copy in small:
        copy.wait()
    rows_r[z, y, core, me] = (weight_v[...] * gain_v[...]).astype(jnp.bfloat16)
    pl.semaphore_wait(barrier, 8)

    first_sums = send_sums(0, CHUNK // BLOCK, 0)
    mine = rows_r.at[z, y, core, me]
    sent = [send(mine, mine, rx_s.at[k], rx_r.at[k], at_x[k]) for k in range(3)]
    for c in range(1, CHUNKS):
        average(c)
    other_sums = send_sums(CHUNK // BLOCK, BLOCKS, 1)

    own = []
    for c in range(CHUNKS):
        if c == 0:
            for copy in first_sums:
                copy.wait_recv()
        if c == 1:
            for copy in other_sums:
                copy.wait_recv()
        narrow(c)
        block = block_of(c, me)
        own.append([send(block, block, own_s.at[k, c], own_r.at[k, c], at_x[k]) for k in range(2)])

    for copy in sent:
        copy.wait_recv()
    line = rows_r.at[z, y, core]
    y_sent = [
        send(line, line, ry_s.at[0], ry_r.at[0], at_y_up),
        send(line, line, ry_s.at[1], ry_r.at[1], at_y_down),
    ]
    for copy in y_sent:
        copy.wait_recv()
    line = rows_r.at[z, y_down, core]
    y_sent.append(send(line, line, ry_s.at[2], ry_r.at[2], at_y_up))
    y_sent[2].wait_recv()
    sent += y_sent
    for step in range(NZ // 2):
        plane = rows_r.at[lax.rem(z + NZ - step, NZ), :, core]
        up = [send(plane, plane, rz_s.at[0, step], rz_r.at[0, step], at_z_up)]
        if step < NZ // 2 - 1:
            plane = rows_r.at[lax.rem(z + step, NZ), :, core]
            up.append(send(plane, plane, rz_s.at[1, step], rz_r.at[1, step], at_z_down))
        for copy in up:
            copy.wait_recv()
        sent += up
    side = rows_r.at[:, :, core]
    sent.append(send(side, side, rc_s, rc_r, at_core))
    sent[-1].wait_recv()

    def widen(i, carry):
        for j in range(NC):
            for x in range(NX):
                piece = rows_r[i // NY, lax.rem(i, NY), j, x].astype(jnp.float32)
                wide_r[i, 2 * j : 2 * j + 2, x * PART : (x + 1) * PART] = piece
        return carry

    lax.fori_loop(0, NZ * NY, widen, 0)

    def turn(i, carry):
        columns = pl.ds(pl.multiple_of(i * 128, 128), 128)
        tile = wide_r[:, :, columns].reshape(128, 128)
        router[columns, :] = tile.T.astype(jnp.bfloat16)
        return carry

    lax.fori_loop(0, D_MODEL // 128, turn, 0)

    far = []
    for c in range(CHUNKS):
        k = 0 if c < HALF else 1
        own[c][k].wait_recv()
        block = block_of(c, left if k == 0 else right)
        far.append(send(block, block, far_s.at[c], far_r.at[c], at_x[k]))
    for c in range(CHUNKS):
        own[c][1 if c < HALF else 0].wait_recv()
    for copy in far:
        copy.wait_recv()
    for copy in (*first_sums, *other_sums, *sent, *(k for pair in own for k in pair), *far):
        copy.wait_send()


def write(ready, scale, router, latest, ready_out, scale_out, router_out, latest_out, sem):
    pieces = [(ready, ready_out, k, ROWS // 6) for k in range(6)]
    pieces += [(latest, latest_out, k, ROWS // 3) for k in range(3)]
    pieces += [(router, router_out, 0, D_MODEL), (scale, scale_out, 0, 2)]
    copies = [
        pltpu.make_async_copy(src.at[pl.ds(k * n, n)], dst.at[pl.ds(k * n, n)], sem.at[i])
        for i, (src, dst, k, n) in enumerate(pieces)
    ]
    for copy in copies:
        copy.start()
    for copy in copies:
        copy.wait()


def shards(train_down, other_down, router_weight, router_gain):
    f32, bf16 = jnp.float32, jnp.bfloat16
    dma = pltpu.SemaphoreType.DMA
    shapes = (((ROWS, D_MODEL), bf16), ((2, ROWS // 2), f32), ((D_MODEL, 128), bf16), ((ROWS, PART), f32))
    given = (
        train_down.reshape(ROWS, PART),
        other_down.reshape(ROWS, PART),
        router_weight.T,
        router_gain.reshape(1, PART),
    )
    made = pl.pallas_call(
        kernel,
        out_shape=tuple(pltpu.VMEM(*k) for k in shapes),
        in_specs=[pl.BlockSpec(memory_space=pltpu.HBM)] * 4,
        out_specs=[pl.BlockSpec(memory_space=pltpu.VMEM)] * 4,
        scratch_shapes=[
            pltpu.VMEM((ROWS, PART), f32),
            pltpu.VMEM((ROWS, PART), f32),
            pltpu.VMEM((2, PART), f32),
            pltpu.VMEM((1, PART), f32),
            pltpu.VMEM((NX, BLOCKS, 1, BLOCK), f32),
            pltpu.VMEM((NZ, NY, NC, NX, 2, PART), bf16),
            pltpu.VMEM((NZ * NY, 2 * NC, D_MODEL), f32),
            dma((2, CHUNKS)), dma((2,)),
            dma((2, 3)), dma((2, 3)),
            dma((3,)), dma((3,)),
            dma((3,)), dma((3,)),
            dma((2, NZ // 2)), dma((2, NZ // 2)),
            dma, dma,
            dma((2, CHUNKS)), dma((2, CHUNKS)),
            dma((CHUNKS,)), dma((CHUNKS,)),
        ],
        compiler_params=pltpu.CompilerParams(
            collective_id=0, has_side_effects=True, vmem_limit_bytes=16 * 2**20
        ),
    )(*(pltpu.with_memory_space_constraint(k, pltpu.HBM) for k in given))
    ready, scale, router, latest = pl.pallas_call(
        write,
        out_shape=tuple(pltpu.HBM(*k) for k in shapes),
        in_specs=[pl.BlockSpec(memory_space=pltpu.VMEM)] * 4,
        out_specs=[pl.BlockSpec(memory_space=pltpu.HBM)] * 4,
        scratch_shapes=[dma((11,))],
        compiler_params=pltpu.CompilerParams(vmem_limit_bytes=2**20),
    )(*made)
    return ready.reshape(2, ROWS // 2, D_MODEL), scale, router, latest.reshape(2, ROWS // 2, PART)


def solution(mesh):
    return jax.shard_map(
        shards,
        mesh=mesh,
        in_specs=(P("bank", None, "zero"), P("bank", None, "zero"), P("zero", "bank"), P("zero")),
        out_specs=(P("bank", None, None), P("bank", None), P(), P("bank", None, "zero")),
        check_vma=False,
    )
```

```python
import functools

import jax
import jax.numpy as jnp
from jax import lax
from jax.experimental import pallas as pl
from jax.experimental.pallas import tpu as pltpu
from jax.sharding import PartitionSpec as P

MESH = pl.DeviceIdType.MESH
D_MODEL = 2048
ROWS = 1536
PART = 512
BLOCK = 128
BLOCKS = ROWS // BLOCK
FILL = 128
FILLS = 4
EARLY = 4
EDGES = (FILL, 256, 512, 768, 1024, 1280, 1536)
CHUNKS = len(EDGES) - 1
FAR = (0, 256, 512, 768, 1024, 1280, 1536)
HALF = 3
READS = (0, 128, 512, 1024, 1536)
NZ, NY, NC, NX = 8, 4, 2, 4


def kernel(
    train, other, weight, gain,
    ready, scale, router, latest,
    train_v, other_v, weight_v, gain_v, sums, fill, rows_r, wide_r,
    z_ready, in_sem, small_sem, sum_s, sum_r, rx_s, rx_r, ry_s, ry_r, rz_s, rz_r, rc_s, rc_r,
    fill_s, fill_r, own_s, own_r, far_s, far_r,
):
    me = lax.axis_index("zero")
    bank = lax.axis_index("bank")
    z, y, core = bank // (NY * NC), lax.rem(bank // NC, NY), lax.rem(bank, NC)
    right, left, opposite = (lax.rem(me + k, NX) for k in (1, 3, 2))
    bank_of = lambda z, y, core: (z * NY + y) * NC + core
    z_up, z_down = lax.rem(z + 1, NZ), lax.rem(z + NZ - 1, NZ)
    y_up, y_down = lax.rem(y + 1, NY), lax.rem(y + NY - 1, NY)
    at_y_up, at_y_down = {"bank": bank_of(z, y_up, core)}, {"bank": bank_of(z, y_down, core)}
    at_z_up, at_z_down = {"bank": bank_of(z_up, y, core)}, {"bank": bank_of(z_down, y, core)}
    at_core = {"bank": bank_of(z, y, 1 - core)}
    at_x = [{"zero": right}, {"zero": left}, {"zero": opposite}]

    even = lax.rem(z, 2) == 0
    barrier = pltpu.get_barrier_semaphore()
    for peer in (*at_x, at_y_up, at_y_down, at_core):
        pl.semaphore_signal(barrier, inc=1, device_id=peer, device_id_type=MESH)

    @pl.when(even)
    def _():
        for peer in (at_z_up, at_z_down):
            pl.semaphore_signal(barrier, inc=1, device_id=peer, device_id_type=MESH)

    def read(c):
        rows = pl.ds(READS[c], READS[c + 1] - READS[c])
        return [
            pltpu.make_async_copy(train.at[rows], train_v.at[rows], in_sem.at[0, c]),
            pltpu.make_async_copy(other.at[rows], other_v.at[rows], in_sem.at[1, c]),
        ]

    small = [
        pltpu.make_async_copy(weight, weight_v, small_sem.at[0]),
        pltpu.make_async_copy(gain, gain_v, small_sem.at[1]),
    ]
    reads = [read(c) for c in range(len(READS) - 1)]
    for copy in (*reads[0], *reads[1], *small, *reads[2], *reads[3]):
        copy.start()

    def send(src, dst, s, r, to):
        copy = pltpu.make_async_remote_copy(
            src_ref=src, dst_ref=dst, send_sem=s, recv_sem=r, device_id=to, device_id_type=MESH
        )
        copy.start()
        return copy

    def average(c):
        for copy in reads[c]:
            copy.wait()
        for b in range(READS[c] // BLOCK, READS[c + 1] // BLOCK):
            rows = pl.ds(b * BLOCK, BLOCK)
            mixed = 0.5 * other_v[rows, :] + 0.5 * train_v[rows, :]
            latest[rows, :] = mixed
            size = jnp.abs(mixed)
            lanes = sum(size[:, k * 128 : (k + 1) * 128] for k in range(1, PART // 128)) + size[:, :128]
            sums[me, b] = jnp.sum(lanes.T, axis=0, keepdims=True)

    def send_sums(first, last, group):
        blocks = pl.ds(first, last - first)
        return [
            send(sums.at[me, blocks], sums.at[me, blocks], sum_s.at[group, k], sum_r.at[group, k], at_x[k])
            for k in (2, 0, 1)
        ]

    def mean(b):
        return ((sums[0, b] + sums[1, b]) + (sums[2, b] + sums[3, b])) / D_MODEL

    def factor(b):
        return jnp.broadcast_to(1.0 / mean(b), (BLOCK, BLOCK)).T

    def narrow(b):
        per = BLOCKS // 2
        rows = pl.ds(b * BLOCK, BLOCK)
        scale[b // per : b // per + 1, (b % per) * BLOCK : (b % per + 1) * BLOCK] = mean(b)
        times = factor(b)
        for k in range(PART // 128):
            columns = pl.ds(pl.multiple_of(me * PART + k * 128, 128), 128)
            ready[rows, columns] = (latest[rows, k * 128 : (k + 1) * 128] * times).astype(jnp.bfloat16)

    def narrow_fill(side, x):
        times = factor(0)[:FILL]
        for k in range(PART // 128):
            columns = pl.ds(pl.multiple_of(x * PART + k * 128, 128), 128)
            ready[:FILL, columns] = (fill[side, :, k * 128 : (k + 1) * 128] * times).astype(jnp.bfloat16)

    def block_of(first, last, x):
        return ready.at[pl.ds(first, last - first), pl.ds(pl.multiple_of(x * PART, PART), PART)]

    def send_fill(i):
        rows = pl.ds(i * (FILL // FILLS), FILL // FILLS)
        return [
            send(latest.at[rows], fill.at[1 - k, rows], fill_s.at[k, i], fill_r.at[k, i], at_x[k])
            for k in range(2)
        ]

    average(0)
    for copy in small:
        copy.wait()
    rows_r[z, y, core, me] = (weight_v[...] * gain_v[...]).astype(jnp.bfloat16)
    pl.semaphore_wait(barrier, 6 + 2 * lax.rem(z, 2))

    @pl.when(jnp.logical_not(even))
    def _():
        for peer in (at_z_up, at_z_down):
            pl.semaphore_signal(z_ready, inc=1, device_id=peer, device_id_type=MESH)

    filled = [send_fill(0)]
    average(1)
    first_sums = send_sums(0, EARLY, 0)
    mine = rows_r.at[z, y, core, me]
    sent = [send(mine, mine, rx_s.at[k], rx_r.at[k], at_x[k]) for k in range(3)]
    filled.append(send_fill(1))
    average(2)
    average(3)
    other_sums = send_sums(EARLY, BLOCKS, 1)
    for i in range(2, FILLS):
        filled.append(send_fill(i))

    own = []
    for copy in first_sums:
        copy.wait_recv()
    for c in range(CHUNKS):
        if EDGES[c] == EARLY * BLOCK:
            narrow(0)
            for copy in other_sums:
                copy.wait_recv()
        for b in range(EDGES[c] // BLOCK, EDGES[c + 1] // BLOCK):
            narrow(b)
        block = block_of(EDGES[c], EDGES[c + 1], me)
        own.append([send(block, block, own_s.at[k, c], own_r.at[k, c], at_x[k]) for k in range(2)])
    for pair in filled:
        for copy in pair:
            copy.wait_recv()
    narrow_fill(0, right)
    narrow_fill(1, left)

    for copy in sent:
        copy.wait_recv()
    line = rows_r.at[z, y, core]
    y_sent = [
        send(line, line, ry_s.at[0], ry_r.at[0], at_y_up),
        send(line, line, ry_s.at[1], ry_r.at[1], at_y_down),
    ]
    for copy in y_sent:
        copy.wait_recv()
    line = rows_r.at[z, y_down, core]
    y_sent.append(send(line, line, ry_s.at[2], ry_r.at[2], at_y_up))
    y_sent[2].wait_recv()
    sent += y_sent

    @pl.when(even)
    def _():
        pl.semaphore_wait(z_ready, 2)

    for step in range(NZ // 2):
        plane = rows_r.at[lax.rem(z + NZ - step, NZ), :, core]
        up = [send(plane, plane, rz_s.at[0, step], rz_r.at[0, step], at_z_up)]
        if step < NZ // 2 - 1:
            plane = rows_r.at[lax.rem(z + step, NZ), :, core]
            up.append(send(plane, plane, rz_s.at[1, step], rz_r.at[1, step], at_z_down))
        for copy in up:
            copy.wait_recv()
        sent += up
    side = rows_r.at[:, :, core]
    sent.append(send(side, side, rc_s, rc_r, at_core))
    sent[-1].wait_recv()

    def widen(i, carry):
        for j in range(NC):
            for x in range(NX):
                piece = rows_r[i // NY, lax.rem(i, NY), j, x].astype(jnp.float32)
                wide_r[i, 2 * j : 2 * j + 2, x * PART : (x + 1) * PART] = piece
        return carry

    lax.fori_loop(0, NZ * NY, widen, 0)

    def turn(i, carry):
        columns = pl.ds(pl.multiple_of(i * 128, 128), 128)
        tile = wide_r[:, :, columns].reshape(128, 128)
        router[columns, :] = tile.T.astype(jnp.bfloat16)
        return carry

    lax.fori_loop(0, D_MODEL // 128, turn, 0)

    far = []
    for c in range(len(FAR) - 1):
        k = 0 if c < HALF else 1
        own[c][k].wait_recv()
        block = block_of(FAR[c], FAR[c + 1], left if k == 0 else right)
        far.append(send(block, block, far_s.at[c], far_r.at[c], at_x[k]))
    for c in range(CHUNKS):
        own[c][1 if c < HALF else 0].wait_recv()
    for copy in far:
        copy.wait_recv()
    for pair in (*filled, *own, first_sums, other_sums, sent, far):
        for copy in pair:
            copy.wait_send()


def write(ready, scale, router, latest, ready_out, scale_out, router_out, latest_out, sem):
    pieces = [(ready, ready_out, k, ROWS // 6) for k in range(6)]
    pieces += [(latest, latest_out, k, ROWS // 3) for k in range(3)]
    pieces += [(router, router_out, 0, D_MODEL), (scale, scale_out, 0, 2)]
    copies = [
        pltpu.make_async_copy(src.at[pl.ds(k * n, n)], dst.at[pl.ds(k * n, n)], sem.at[i])
        for i, (src, dst, k, n) in enumerate(pieces)
    ]
    for copy in copies:
        copy.start()
    for copy in copies:
        copy.wait()


def shards(train_down, other_down, router_weight, router_gain):
    f32, bf16 = jnp.float32, jnp.bfloat16
    dma = pltpu.SemaphoreType.DMA
    shapes = (((ROWS, D_MODEL), bf16), ((2, ROWS // 2), f32), ((D_MODEL, 128), bf16), ((ROWS, PART), f32))
    given = (
        train_down.reshape(ROWS, PART),
        other_down.reshape(ROWS, PART),
        router_weight.T,
        router_gain.reshape(1, PART),
    )
    made = pl.pallas_call(
        kernel,
        out_shape=tuple(pltpu.VMEM(*k) for k in shapes),
        in_specs=[pl.BlockSpec(memory_space=pltpu.HBM)] * 4,
        out_specs=[pl.BlockSpec(memory_space=pltpu.VMEM)] * 4,
        scratch_shapes=[
            pltpu.VMEM((ROWS, PART), f32),
            pltpu.VMEM((ROWS, PART), f32),
            pltpu.VMEM((2, PART), f32),
            pltpu.VMEM((1, PART), f32),
            pltpu.VMEM((NX, BLOCKS, 1, BLOCK), f32),
            pltpu.VMEM((2, FILL, PART), f32),
            pltpu.VMEM((NZ, NY, NC, NX, 2, PART), bf16),
            pltpu.VMEM((NZ * NY, 2 * NC, D_MODEL), f32),
            pltpu.SemaphoreType.REGULAR,
            dma((2, len(READS) - 1)), dma((2,)),
            dma((2, 3)), dma((2, 3)),
            dma((3,)), dma((3,)),
            dma((3,)), dma((3,)),
            dma((2, NZ // 2)), dma((2, NZ // 2)),
            dma, dma,
            dma((2, FILLS)), dma((2, FILLS)),
            dma((2, CHUNKS)), dma((2, CHUNKS)),
            dma((len(FAR) - 1,)), dma((len(FAR) - 1,)),
        ],
        compiler_params=pltpu.CompilerParams(
            collective_id=0, has_side_effects=True, vmem_limit_bytes=16 * 2**20
        ),
    )(*(pltpu.with_memory_space_constraint(k, pltpu.HBM) for k in given))
    ready, scale, router, latest = pl.pallas_call(
        write,
        out_shape=tuple(pltpu.HBM(*k) for k in shapes),
        in_specs=[pl.BlockSpec(memory_space=pltpu.VMEM)] * 4,
        out_specs=[pl.BlockSpec(memory_space=pltpu.HBM)] * 4,
        scratch_shapes=[dma((11,))],
        compiler_params=pltpu.CompilerParams(vmem_limit_bytes=2**20),
    )(*made)
    return ready.reshape(2, ROWS // 2, D_MODEL), scale, router, latest.reshape(2, ROWS // 2, PART)


def solution(mesh):
    return jax.shard_map(
        shards,
        mesh=mesh,
        in_specs=(P("bank", None, "zero"), P("bank", None, "zero"), P("zero", "bank"), P("zero")),
        out_specs=(P("bank", None, None), P("bank", None), P(), P("bank", None, "zero")),
        check_vma=False,
    )
```

```python
import functools

import jax
import jax.numpy as jnp
from jax import lax
from jax.experimental import pallas as pl
from jax.experimental.pallas import tpu as pltpu
from jax.sharding import PartitionSpec as P

MESH = pl.DeviceIdType.MESH
D_MODEL = 2048
ROWS = 1536
PART = 512
BLOCK = 128
BLOCKS = ROWS // BLOCK
FILL = 64
FILLS = 1
READS = (0, 128, 256, 512, 1024, 1536)
EARLY = 2
EDGES = (FILL, 128, 256, 512, 768, 1024, 1280, 1536)
CHUNKS = len(EDGES) - 1
FAR = (0, 256, 512, 768, 1024, 1280, 1536)
ORDERS = (0, 1, 2, 3, 4, 5, 6), (0, 1, 4, 5, 6, 2, 3)
NZ, NY, NC, NX = 8, 4, 2, 4


def kernel(
    train, other, weight, gain,
    ready, scale, router, latest,
    train_v, other_v, weight_v, gain_v, sums, fill, rows_r, wide_r,
    line_ready, z_ready, go, in_sem, small_sem, sum_s, sum_r, rx_s, rx_r, ry_s, ry_r, rz_s, rz_r, rc_s, rc_r,
    fill_s, fill_r, own_s, own_r, far_s, far_r,
):
    me = lax.axis_index("zero")
    bank = lax.axis_index("bank")
    z, y, core = bank // (NY * NC), lax.rem(bank // NC, NY), lax.rem(bank, NC)
    right, left, opposite = (lax.rem(me + k, NX) for k in (1, 3, 2))
    bank_of = lambda z, y, core: (z * NY + y) * NC + core
    z_up, z_down = lax.rem(z + 1, NZ), lax.rem(z + NZ - 1, NZ)
    y_up, y_down = lax.rem(y + 1, NY), lax.rem(y + NY - 1, NY)
    at_y_up, at_y_down = {"bank": bank_of(z, y_up, core)}, {"bank": bank_of(z, y_down, core)}
    at_z_up, at_z_down = {"bank": bank_of(z_up, y, core)}, {"bank": bank_of(z_down, y, core)}
    at_core = {"bank": bank_of(z, y, 1 - core)}
    at_x = [{"zero": right}, {"zero": left}, {"zero": opposite}]

    lead = me == 0
    even = lax.rem(z, 2) == 0
    near, above = (at_y_up, at_y_down, at_core), (at_z_up, at_z_down)
    barrier = pltpu.get_barrier_semaphore()

    def tell(peers, semaphore):
        for peer in peers:
            pl.semaphore_signal(semaphore, inc=1, device_id=peer, device_id_type=MESH)

    tell(at_x, barrier)

    @pl.when(lead)
    def _():
        tell(near, barrier)

    @pl.when(lead & even)
    def _():
        tell(above, barrier)

    def read(c):
        rows = pl.ds(READS[c], READS[c + 1] - READS[c])
        return [
            pltpu.make_async_copy(train.at[rows], train_v.at[rows], in_sem.at[0, c]),
            pltpu.make_async_copy(other.at[rows], other_v.at[rows], in_sem.at[1, c]),
        ]

    small = [
        pltpu.make_async_copy(weight, weight_v, small_sem.at[0]),
        pltpu.make_async_copy(gain, gain_v, small_sem.at[1]),
    ]
    reads = [read(c) for c in range(len(READS) - 1)]
    for copy in (*small, *reads[0], *reads[1]):
        copy.start()

    def send(src, dst, s, r, to):
        copy = pltpu.make_async_remote_copy(
            src_ref=src, dst_ref=dst, send_sem=s, recv_sem=r, device_id=to, device_id_type=MESH
        )
        copy.start()
        return copy

    def average(c):
        for copy in reads[c]:
            copy.wait()
        for b in range(READS[c] // BLOCK, READS[c + 1] // BLOCK):
            rows = pl.ds(b * BLOCK, BLOCK)
            mixed = 0.5 * other_v[rows, :] + 0.5 * train_v[rows, :]
            latest[rows, :] = mixed
            size = jnp.abs(mixed)
            lanes = sum(size[:, k * 128 : (k + 1) * 128] for k in range(1, PART // 128)) + size[:, :128]
            sums[me, b] = jnp.sum(lanes.T, axis=0, keepdims=True)

    def send_sums(first, last, group):
        blocks = pl.ds(first, last - first)
        return [
            send(sums.at[me, blocks], sums.at[me, blocks], sum_s.at[group, k], sum_r.at[group, k], at_x[k])
            for k in (2, 0, 1)
        ]

    def mean(b):
        return ((sums[0, b] + sums[1, b]) + (sums[2, b] + sums[3, b])) / D_MODEL

    def factor(b):
        return jnp.broadcast_to(1.0 / mean(b), (BLOCK, BLOCK)).T

    def narrow(b):
        per = BLOCKS // 2
        rows = pl.ds(b * BLOCK, BLOCK)
        scale[b // per : b // per + 1, (b % per) * BLOCK : (b % per + 1) * BLOCK] = mean(b)
        times = factor(b)
        for k in range(PART // 128):
            columns = pl.ds(pl.multiple_of(me * PART + k * 128, 128), 128)
            ready[rows, columns] = (latest[rows, k * 128 : (k + 1) * 128] * times).astype(jnp.bfloat16)

    def narrow_fill(side, x):
        times = factor(0)[:FILL]
        for k in range(PART // 128):
            columns = pl.ds(pl.multiple_of(x * PART + k * 128, 128), 128)
            ready[:FILL, columns] = (fill[side, :, k * 128 : (k + 1) * 128] * times).astype(jnp.bfloat16)

    def block_of(first, last, x):
        return ready.at[pl.ds(first, last - first), pl.ds(pl.multiple_of(x * PART, PART), PART)]

    def send_fill(i):
        rows = pl.ds(i * (FILL // FILLS), FILL // FILLS)
        return [
            send(latest.at[rows], fill.at[1 - k, rows], fill_s.at[k, i], fill_r.at[k, i], at_x[k])
            for k in range(2)
        ]

    average(0)
    for pair in reads[EARLY:]:
        for copy in pair:
            copy.start()
    average(1)
    for copy in small:
        copy.wait()
    rows_r[z, y, core, me] = (weight_v[...] * gain_v[...]).astype(jnp.bfloat16)
    pl.semaphore_wait(barrier, jnp.where(lead, 6 + 2 * lax.rem(z, 2), 3))

    first_sums = send_sums(0, READS[EARLY] // BLOCK, 0)
    mine = rows_r.at[z, y, core, me]
    sent = [send(mine, mine, rx_s.at[k], rx_r.at[k], at_x[k]) for k in range(3)]
    filled = [send_fill(0)]

    @pl.when(lead)
    def _():
        tell(near, line_ready)

    @pl.when(lead & jnp.logical_not(even))
    def _():
        tell(above, line_ready)

    for c in range(EARLY, len(READS) - 1):
        average(c)
    other_sums = send_sums(READS[EARLY] // BLOCK, BLOCKS, 1)
    for i in range(1, FILLS):
        filled.append(send_fill(i))

    own = {}
    for copy in first_sums:
        copy.wait_recv()
    narrowed, done = READS[EARLY], set()
    for order in zip(*ORDERS):
        for k, c in enumerate(order):
            if EDGES[c + 1] > narrowed == READS[EARLY]:
                for copy in other_sums:
                    copy.wait_recv()
                narrowed = ROWS
            for b in range(EDGES[c] // BLOCK, EDGES[c + 1] // BLOCK):
                if b not in done:
                    done.add(b)
                    narrow(b)
            block = block_of(EDGES[c], EDGES[c + 1], me)
            own[k, c] = send(block, block, own_s.at[k, c], own_r.at[k, c], at_x[k])
    for pair in filled:
        for copy in pair:
            copy.wait_recv()
    narrow_fill(0, right)
    narrow_fill(1, left)

    far, held = [], set(own)

    def take(k, first, last):
        for c in range(CHUNKS):
            if (k, c) in held and EDGES[c] < last and EDGES[c + 1] > first:
                held.remove((k, c))
                own[k, c].wait_recv()

    def pass_on(*chunks):
        for c in chunks:
            k = 0 if FAR[c] < ROWS // 2 else 1
            take(k, FAR[c], FAR[c + 1])
            block = block_of(FAR[c], FAR[c + 1], left if k == 0 else right)
            far.append(send(block, block, far_s.at[c], far_r.at[c], at_x[k]))

    @pl.when(lead & even)
    def _():
        pl.semaphore_wait(line_ready, 5)
        tell(above, z_ready)

    @pl.when(lead & jnp.logical_not(even))
    def _():
        pl.semaphore_wait(line_ready, 3)
        pl.semaphore_wait(z_ready, 2)

    @pl.when(lead)
    def _():
        tell(at_x, go)

    @pl.when(jnp.logical_not(lead))
    def _():
        pl.semaphore_wait(go, 1)

    for copy in sent:
        copy.wait_recv()
    line = rows_r.at[z, y, core]
    y_sent = [
        send(line, line, ry_s.at[0], ry_r.at[0], at_y_up),
        send(line, line, ry_s.at[1], ry_r.at[1], at_y_down),
    ]
    for copy in y_sent:
        copy.wait_recv()
    line = rows_r.at[z, y_down, core]
    y_sent.append(send(line, line, ry_s.at[2], ry_r.at[2], at_y_up))
    y_sent[2].wait_recv()
    sent += y_sent
    pass_on(0, 3)

    for step in range(NZ // 2):
        plane = rows_r.at[lax.rem(z + NZ - step, NZ), :, core]
        up = [send(plane, plane, rz_s.at[0, step], rz_r.at[0, step], at_z_up)]
        if step < NZ // 2 - 1:
            plane = rows_r.at[lax.rem(z + step, NZ), :, core]
            up.append(send(plane, plane, rz_s.at[1, step], rz_r.at[1, step], at_z_down))
        for copy in up:
            copy.wait_recv()
        sent += up
        if step % 2 == 1:
            pass_on(step // 2 + 1, step // 2 + 4)
    side = rows_r.at[:, :, core]
    sent.append(send(side, side, rc_s, rc_r, at_core))
    sent[-1].wait_recv()

    def widen(i, carry):
        for j in range(NC):
            for x in range(NX):
                piece = rows_r[i // NY, lax.rem(i, NY), j, x].astype(jnp.float32)
                wide_r[i, 2 * j : 2 * j + 2, x * PART : (x + 1) * PART] = piece
        return carry

    lax.fori_loop(0, NZ * NY, widen, 0)

    def turn(i, carry):
        columns = pl.ds(pl.multiple_of(i * 128, 128), 128)
        tile = wide_r[:, :, columns].reshape(128, 128)
        router[columns, :] = tile.T.astype(jnp.bfloat16)
        return carry

    lax.fori_loop(0, D_MODEL // 128, turn, 0)

    for k in range(2):
        take(k, 0, ROWS)
    for copy in far:
        copy.wait_recv()
    for pair in (*filled, own.values(), first_sums, other_sums, sent, far):
        for copy in pair:
            copy.wait_send()


def write(ready, scale, router, latest, ready_out, scale_out, router_out, latest_out, sem):
    pieces = [(ready, ready_out, k, ROWS // 6) for k in range(6)]
    pieces += [(latest, latest_out, k, ROWS // 3) for k in range(3)]
    pieces += [(router, router_out, 0, D_MODEL), (scale, scale_out, 0, 2)]
    copies = [
        pltpu.make_async_copy(src.at[pl.ds(k * n, n)], dst.at[pl.ds(k * n, n)], sem.at[i])
        for i, (src, dst, k, n) in enumerate(pieces)
    ]
    for copy in copies:
        copy.start()
    for copy in copies:
        copy.wait()


def shards(train_down, other_down, router_weight, router_gain):
    f32, bf16 = jnp.float32, jnp.bfloat16
    dma = pltpu.SemaphoreType.DMA
    shapes = (((ROWS, D_MODEL), bf16), ((2, ROWS // 2), f32), ((D_MODEL, 128), bf16), ((ROWS, PART), f32))
    given = (
        train_down.reshape(ROWS, PART),
        other_down.reshape(ROWS, PART),
        router_weight.T,
        router_gain.reshape(1, PART),
    )
    made = pl.pallas_call(
        kernel,
        out_shape=tuple(pltpu.VMEM(*k) for k in shapes),
        in_specs=[pl.BlockSpec(memory_space=pltpu.HBM)] * 4,
        out_specs=[pl.BlockSpec(memory_space=pltpu.VMEM)] * 4,
        scratch_shapes=[
            pltpu.VMEM((ROWS, PART), f32),
            pltpu.VMEM((ROWS, PART), f32),
            pltpu.VMEM((2, PART), f32),
            pltpu.VMEM((1, PART), f32),
            pltpu.VMEM((NX, BLOCKS, 1, BLOCK), f32),
            pltpu.VMEM((2, FILL, PART), f32),
            pltpu.VMEM((NZ, NY, NC, NX, 2, PART), bf16),
            pltpu.VMEM((NZ * NY, 2 * NC, D_MODEL), f32),
            *[pltpu.SemaphoreType.REGULAR] * 3,
            dma((2, len(READS) - 1)), dma((2,)),
            dma((2, 3)), dma((2, 3)),
            dma((3,)), dma((3,)),
            dma((3,)), dma((3,)),
            dma((2, NZ // 2)), dma((2, NZ // 2)),
            dma, dma,
            dma((2, FILLS)), dma((2, FILLS)),
            dma((2, CHUNKS)), dma((2, CHUNKS)),
            dma((len(FAR) - 1,)), dma((len(FAR) - 1,)),
        ],
        compiler_params=pltpu.CompilerParams(
            collective_id=0, has_side_effects=True, vmem_limit_bytes=16 * 2**20
        ),
    )(*(pltpu.with_memory_space_constraint(k, pltpu.HBM) for k in given))
    ready, scale, router, latest = pl.pallas_call(
        write,
        out_shape=tuple(pltpu.HBM(*k) for k in shapes),
        in_specs=[pl.BlockSpec(memory_space=pltpu.VMEM)] * 4,
        out_specs=[pl.BlockSpec(memory_space=pltpu.HBM)] * 4,
        scratch_shapes=[dma((11,))],
        compiler_params=pltpu.CompilerParams(vmem_limit_bytes=2**20),
    )(*made)
    return ready.reshape(2, ROWS // 2, D_MODEL), scale, router, latest.reshape(2, ROWS // 2, PART)


def solution(mesh):
    return jax.shard_map(
        shards,
        mesh=mesh,
        in_specs=(P("bank", None, "zero"), P("bank", None, "zero"), P("zero", "bank"), P("zero")),
        out_specs=(P("bank", None, None), P("bank", None), P(), P("bank", None, "zero")),
        check_vma=False,
    )
```

```python
import jax
import jax.numpy as jnp
from jax import lax
from jax.experimental import pallas as pl
from jax.experimental.pallas import tpu as pltpu
from jax.sharding import PartitionSpec as P

MESH = pl.DeviceIdType.MESH
D_MODEL = 2048
ROWS = 1536
PART = 512
BLOCK = 128
BLOCKS = ROWS // BLOCK
FILL = (48, 64)
READS = (0, 128, 256, 768, 1536)
EARLY = 256
HALF = ROWS // 2
NZ, NY, NC, NX = 8, 4, 2, 4


def kernel(
    train, other, weight, gain,
    ready, scale, router, latest,
    given_v, weight_v, gain_v, sums, fill, rows_r, wide_r,
    clear, in_sem, small_sem, out_sem, sum_r, x_r, y_r, z_r, core_r, first_r, pass_r, last_r,
):
    me = lax.axis_index("zero")
    bank = lax.axis_index("bank")
    z, y, core = bank // (NY * NC), lax.rem(bank // NC, NY), lax.rem(bank, NC)
    right, left, opposite = (lax.rem(me + k, NX) for k in (1, 3, 2))
    bank_of = lambda z, y, core: (z * NY + y) * NC + core
    z_up, z_down = lax.rem(z + 1, NZ), lax.rem(z + NZ - 1, NZ)
    y_up, y_down = lax.rem(y + 1, NY), lax.rem(y + NY - 1, NY)
    at_y_up, at_y_down = {"bank": bank_of(z, y_up, core)}, {"bank": bank_of(z, y_down, core)}
    at_z_up, at_z_down = {"bank": bank_of(z_up, y, core)}, {"bank": bank_of(z_down, y, core)}
    at_core = {"bank": bank_of(z, y, 1 - core)}
    at_x = [{"zero": right}, {"zero": left}, {"zero": opposite}]
    lead = me == 0
    even = lax.rem(z, 2) == 0
    near, above = (at_y_up, at_y_down, at_core), (at_z_up, at_z_down)
    barrier = pltpu.get_barrier_semaphore()

    def tell(peers, semaphore):
        for peer in peers:
            pl.semaphore_signal(semaphore, inc=1, device_id=peer, device_id_type=MESH)

    tell(at_x, barrier)

    @pl.when(lead)
    def _():
        tell(near, barrier)

    @pl.when(lead & even)
    def _():
        tell(above, barrier)

    def start_read(c):
        first, last = READS[c], READS[c + 1]
        for k, source in enumerate((train, other)):
            pltpu.make_async_copy(
                source.at[first:last], given_v.at[k * ROWS + first : k * ROWS + last], in_sem.at[c]
            ).start()

    def wait(size, semaphore):
        pltpu.make_async_copy(size, size, semaphore).wait()

    small = [
        pltpu.make_async_copy(weight, weight_v, small_sem.at[0]),
        pltpu.make_async_copy(gain, gain_v, small_sem.at[1]),
    ]
    for copy in small:
        copy.start()
    start_read(0)
    start_read(1)

    def send(src, dst, r, to):
        pltpu.make_async_remote_copy(
            src_ref=src, dst_ref=dst, send_sem=out_sem, recv_sem=r, device_id=to, device_id_type=MESH
        ).start()

    def average(c):
        wait(given_v.at[: 2 * (READS[c + 1] - READS[c])], in_sem.at[c])
        for b in range(READS[c] // BLOCK, READS[c + 1] // BLOCK):
            first, last = b * BLOCK, (b + 1) * BLOCK
            mixed = 0.5 * given_v[ROWS + first : ROWS + last, :] + 0.5 * given_v[first:last, :]
            latest[first:last, :] = mixed
            size = jnp.abs(mixed)
            lanes = sum(size[:, k * 128 : (k + 1) * 128] for k in range(1, PART // 128)) + size[:, :128]
            sums[me, b] = jnp.sum(lanes.T, axis=0, keepdims=True)

    def sums_of(x, group):
        first, last = ((0, EARLY), (EARLY, ROWS))[group]
        return sums.at[x, first // BLOCK : last // BLOCK]

    def send_sums(group):
        for k in (2, 0, 1):
            send(sums_of(me, group), sums_of(me, group), sum_r.at[group], at_x[k])

    def wait_sums(group):
        wait(sums_of(slice(0, NX - 1), group), sum_r.at[group])

    def mean(b):
        return ((sums[0, b] + sums[1, b]) + (sums[2, b] + sums[3, b])) / D_MODEL

    def factor(b):
        return jnp.broadcast_to(1.0 / mean(b), (BLOCK, BLOCK)).T

    def narrow(first, last):
        for b in range(first // BLOCK, last // BLOCK):
            rows = pl.ds(b * BLOCK, BLOCK)
            per = BLOCKS // 2
            scale[b // per : b // per + 1, (b % per) * BLOCK : (b % per + 1) * BLOCK] = mean(b)
            times = factor(b)
            for k in range(PART // 128):
                columns = pl.ds(pl.multiple_of(me * PART + k * 128, 128), 128)
                ready[rows, columns] = (latest[rows, k * 128 : (k + 1) * 128] * times).astype(jnp.bfloat16)

    def narrow_fill(side, x, rows):
        times = factor(0)[:rows]
        for k in range(PART // 128):
            columns = pl.ds(pl.multiple_of(x * PART + k * 128, 128), 128)
            ready[:rows, columns] = (fill[side, :rows, k * 128 : (k + 1) * 128] * times).astype(jnp.bfloat16)

    def block_of(first, last, x):
        return ready.at[pl.ds(first, last - first), pl.ds(pl.multiple_of(x * PART, PART), PART)]

    def send_block(first, last, x, r, k):
        block = block_of(first, last, x)
        send(block, block, r, at_x[k])

    def by_core(act):
        for i, rows in enumerate(FILL):

            @pl.when(core == i)
            def _():
                act(rows)

    def send_fill(rows):
        for k in range(2):
            send(latest.at[:rows], fill.at[1 - k, :rows], first_r, at_x[k])

    def send_first(rows):
        for k in range(2):
            send_block(rows, BLOCK, me, first_r, k)

    def take_first(rows):
        wait(given_v.at[: BLOCK + rows], first_r)
        narrow_fill(0, right, rows)
        narrow_fill(1, left, rows)

    average(0)
    for c in range(2, len(READS) - 1):
        start_read(c)
    average(1)
    for copy in small:
        copy.wait()
    rows_r[z, y, core, me] = (weight_v[...] * gain_v[...]).astype(jnp.bfloat16)
    pl.semaphore_wait(barrier, jnp.where(lead, 6 + 2 * lax.rem(z, 2), 3))

    send_sums(0)
    by_core(send_fill)
    mine = rows_r.at[z, y, core, me]
    for k in range(3):
        send(mine, mine, x_r, at_x[k])

    @pl.when(lead)
    def _():
        tell(near, clear)

    @pl.when(lead & jnp.logical_not(even))
    def _():
        tell(above, clear)

    for c in range(2, len(READS) - 1):
        average(c)
    send_sums(1)

    wait_sums(0)
    narrow(0, BLOCK)
    by_core(send_first)
    narrow(BLOCK, EARLY)
    send_block(BLOCK, EARLY, me, pass_r.at[0], 0)
    send_block(BLOCK, EARLY, me, last_r, 1)
    wait_sums(1)
    narrow(EARLY, HALF)
    send_block(EARLY, HALF, me, pass_r.at[0], 0)
    narrow(HALF, ROWS)
    send_block(HALF, ROWS, me, pass_r.at[1], 1)
    send_block(HALF, ROWS, me, last_r, 0)
    send_block(EARLY, HALF, me, last_r, 1)
    by_core(take_first)

    @pl.when(lead)
    def _():
        pl.semaphore_wait(clear, 5)
        tell(at_x, clear)

    @pl.when(lead & even)
    def _():
        tell(above, clear)

    @pl.when(jnp.logical_not(lead))
    def _():
        pl.semaphore_wait(clear, 1)

    wait(rows_r.at[z, y, core, : NX - 1], x_r)
    line = rows_r.at[z, y, core]
    send(line, line, y_r.at[0], at_y_up)
    send(line, line, y_r.at[0], at_y_down)
    wait(rows_r.at[z, :2, core], y_r.at[0])
    line = rows_r.at[z, y_down, core]
    send(line, line, y_r.at[1], at_y_up)
    wait(line, y_r.at[1])

    for step in range(NZ // 2):
        plane = rows_r.at[lax.rem(z + NZ - step, NZ), :, core]
        send(plane, plane, z_r.at[step], at_z_up)
        if step < NZ // 2 - 1:
            plane = rows_r.at[lax.rem(z + step, NZ), :, core]
            send(plane, plane, z_r.at[step], at_z_down)
            wait(rows_r.at[:2, :, core], z_r.at[step])
        else:
            wait(plane, z_r.at[step])

    wait(block_of(BLOCK, HALF, left), pass_r.at[0])
    send_block(0, HALF, left, last_r, 0)
    wait(block_of(HALF, ROWS, right), pass_r.at[1])
    send_block(HALF, ROWS, right, last_r, 1)

    side = rows_r.at[:, :, core]
    send(side, side, core_r, at_core)
    wait(side, core_r)

    def widen(i, carry):
        for j in range(NC):
            for x in range(NX):
                piece = rows_r[i // NY, lax.rem(i, NY), j, x].astype(jnp.float32)
                wide_r[i, 2 * j : 2 * j + 2, x * PART : (x + 1) * PART] = piece
        return carry

    lax.fori_loop(0, NZ * NY, widen, 0)

    def turn(i, carry):
        columns = pl.ds(pl.multiple_of(i * 128, 128), 128)
        tile = wide_r[:, :, columns].reshape(128, 128)
        router[columns, :] = tile.T.astype(jnp.bfloat16)
        return carry

    lax.fori_loop(0, D_MODEL // 128, turn, 0)

    wait(given_v.at[: ((ROWS - HALF) + (HALF - BLOCK) + 2 * HALF) // 2], last_r)

    def end(rows):
        blocks = 2 * (ROWS - BLOCK) + 2 * HALF + 2 * (BLOCK + rows)
        sums_and_router = 3 * BLOCKS // 2 + 3 * 2 + 3 * 8 + 7 * 32 + 256
        wait(given_v.at[: (blocks + sums_and_router) // 2], out_sem)

    by_core(end)


def write(ready, scale, router, latest, ready_out, scale_out, router_out, latest_out, sem):
    pairs = (ready, ready_out), (latest, latest_out), (router, router_out), (scale, scale_out)
    copies = [pltpu.make_async_copy(src, dst, sem.at[i]) for i, (src, dst) in enumerate(pairs)]
    for copy in copies:
        copy.start()
    for copy in copies:
        copy.wait()


def shards(train_down, other_down, router_weight, router_gain):
    f32, bf16 = jnp.float32, jnp.bfloat16
    dma = pltpu.SemaphoreType.DMA
    shapes = (((ROWS, D_MODEL), bf16), ((2, ROWS // 2), f32), ((D_MODEL, 128), bf16), ((ROWS, PART), f32))
    given = (
        train_down.reshape(ROWS, PART),
        other_down.reshape(ROWS, PART),
        router_weight.T,
        router_gain.reshape(1, PART),
    )
    made = pl.pallas_call(
        kernel,
        out_shape=tuple(pltpu.VMEM(*k) for k in shapes),
        in_specs=[pl.BlockSpec(memory_space=pltpu.HBM)] * 4,
        out_specs=[pl.BlockSpec(memory_space=pltpu.VMEM)] * 4,
        scratch_shapes=[
            pltpu.VMEM((2 * ROWS, PART), f32),
            pltpu.VMEM((2, PART), f32),
            pltpu.VMEM((1, PART), f32),
            pltpu.VMEM((NX, BLOCKS, 1, BLOCK), f32),
            pltpu.VMEM((2, max(FILL), PART), f32),
            pltpu.VMEM((NZ, NY, NC, NX, 2, PART), bf16),
            pltpu.VMEM((NZ * NY, 2 * NC, D_MODEL), f32),
            pltpu.SemaphoreType.REGULAR,
            dma((len(READS) - 1,)), dma((2,)), dma, dma((2,)), dma, dma((2,)), dma((NZ // 2,)), dma, dma, dma((2,)), dma,
        ],
        compiler_params=pltpu.CompilerParams(
            collective_id=0, has_side_effects=True, vmem_limit_bytes=16 * 2**20
        ),
    )(*(pltpu.with_memory_space_constraint(k, pltpu.HBM) for k in given))
    ready, scale, router, latest = pl.pallas_call(
        write,
        out_shape=tuple(pltpu.HBM(*k) for k in shapes),
        in_specs=[pl.BlockSpec(memory_space=pltpu.VMEM)] * 4,
        out_specs=[pl.BlockSpec(memory_space=pltpu.HBM)] * 4,
        scratch_shapes=[dma((4,))],
        compiler_params=pltpu.CompilerParams(vmem_limit_bytes=2**20),
    )(*made)
    return ready.reshape(2, ROWS // 2, D_MODEL), scale, router, latest.reshape(2, ROWS // 2, PART)


def solution(mesh):
    return jax.shard_map(
        shards,
        mesh=mesh,
        in_specs=(P("bank", None, "zero"), P("bank", None, "zero"), P("zero", "bank"), P("zero")),
        out_specs=(P("bank", None, None), P("bank", None), P(), P("bank", None, "zero")),
        check_vma=False,
    )
```

```python
import jax
import jax.numpy as jnp
from jax import lax
from jax.experimental import pallas as pl
from jax.experimental.pallas import tpu as pltpu
from jax.sharding import PartitionSpec as P

MESH = pl.DeviceIdType.MESH
D_MODEL = 2048
ROWS = 1536
PART = 512
BLOCK = 128
BLOCKS = ROWS // BLOCK
FILL = (48, 64)
READS = (0, 128, 256, 768, 1536)
EARLY = 256
HALF = ROWS // 2
SHIFT = 32
NZ, NY, NC, NX = 8, 4, 2, 4


def kernel(
    train, other, weight, gain,
    ready, scale, router, latest,
    given_v, weight_v, gain_v, sums, fill, rows_r, wide_r,
    clear, in_sem, small_sem, out_sem, sum_r, x_r, y_r, z_r, core_r, first_r, pass_r, last_r,
):
    me = lax.axis_index("zero")
    bank = lax.axis_index("bank")
    z, y, core = bank // (NY * NC), lax.rem(bank // NC, NY), lax.rem(bank, NC)
    right, left, opposite = (lax.rem(me + k, NX) for k in (1, 3, 2))
    bank_of = lambda z, y, core: (z * NY + y) * NC + core
    z_up, z_down = lax.rem(z + 1, NZ), lax.rem(z + NZ - 1, NZ)
    y_up, y_down = lax.rem(y + 1, NY), lax.rem(y + NY - 1, NY)
    at_y_up, at_y_down = {"bank": bank_of(z, y_up, core)}, {"bank": bank_of(z, y_down, core)}
    at_z_up, at_z_down = {"bank": bank_of(z_up, y, core)}, {"bank": bank_of(z_down, y, core)}
    at_core = {"bank": bank_of(z, y, 1 - core)}
    at_x = [{"zero": right}, {"zero": left}, {"zero": opposite}]
    lead = me == 0
    even = lax.rem(z, 2) == 0
    near, above = (at_y_up, at_y_down, at_core), (at_z_up, at_z_down)
    barrier = pltpu.get_barrier_semaphore()

    def tell(peers, semaphore):
        for peer in peers:
            pl.semaphore_signal(semaphore, inc=1, device_id=peer, device_id_type=MESH)

    tell(at_x, barrier)

    @pl.when(lead)
    def _():
        tell(near, barrier)

    @pl.when(lead & even)
    def _():
        tell(above, barrier)

    def start_read(c):
        first, last = READS[c], READS[c + 1]
        for k, source in enumerate((train, other)):
            pltpu.make_async_copy(
                source.at[first:last], given_v.at[k * ROWS + first : k * ROWS + last], in_sem.at[c]
            ).start()

    def wait(size, semaphore):
        pltpu.make_async_copy(size, size, semaphore).wait()

    small = [
        pltpu.make_async_copy(weight, weight_v, small_sem.at[0]),
        pltpu.make_async_copy(gain, gain_v, small_sem.at[1]),
    ]
    for copy in small:
        copy.start()
    start_read(0)
    start_read(1)

    def send(src, dst, r, to):
        pltpu.make_async_remote_copy(
            src_ref=src, dst_ref=dst, send_sem=out_sem, recv_sem=r, device_id=to, device_id_type=MESH
        ).start()

    def average(c):
        wait(given_v.at[: 2 * (READS[c + 1] - READS[c])], in_sem.at[c])
        for b in range(READS[c] // BLOCK, READS[c + 1] // BLOCK):
            first, last = b * BLOCK, (b + 1) * BLOCK
            mixed = 0.5 * given_v[ROWS + first : ROWS + last, :] + 0.5 * given_v[first:last, :]
            latest[first:last, :] = mixed
            size = jnp.abs(mixed)
            lanes = sum(size[:, k * 128 : (k + 1) * 128] for k in range(1, PART // 128)) + size[:, :128]
            sums[me, b] = jnp.sum(lanes.T, axis=0, keepdims=True)

    def sums_of(x, group):
        first, last = ((0, EARLY), (EARLY, ROWS))[group]
        return sums.at[x, first // BLOCK : last // BLOCK]

    def send_sums(group):
        for k in (2, 0, 1):
            send(sums_of(me, group), sums_of(me, group), sum_r.at[group], at_x[k])

    def wait_sums(group):
        wait(sums_of(slice(0, NX - 1), group), sum_r.at[group])

    def mean(b):
        return ((sums[0, b] + sums[1, b]) + (sums[2, b] + sums[3, b])) / D_MODEL

    def factor(b):
        return jnp.broadcast_to(1.0 / mean(b), (BLOCK, BLOCK)).T

    def narrow(first, last):
        for b in range(first // BLOCK, last // BLOCK):
            rows = pl.ds(b * BLOCK, BLOCK)
            per = BLOCKS // 2
            scale[b // per : b // per + 1, (b % per) * BLOCK : (b % per + 1) * BLOCK] = mean(b)
            times = factor(b)
            for k in range(PART // 128):
                columns = pl.ds(pl.multiple_of(me * PART + k * 128, 128), 128)
                ready[rows, columns] = (latest[rows, k * 128 : (k + 1) * 128] * times).astype(jnp.bfloat16)

    def narrow_fill(side, x, rows):
        times = factor(0)[:rows]
        for k in range(PART // 128):
            columns = pl.ds(pl.multiple_of(x * PART + k * 128, 128), 128)
            ready[:rows, columns] = (fill[side, :rows, k * 128 : (k + 1) * 128] * times).astype(jnp.bfloat16)

    def block_of(first, last, x):
        return ready.at[pl.ds(first, last - first), pl.ds(pl.multiple_of(x * PART, PART), PART)]

    def send_block(first, last, x, r, k):
        block = block_of(first, last, x)
        send(block, block, r, at_x[k])

    def by_core(act):
        for i, rows in enumerate(FILL):

            @pl.when(core == i)
            def _():
                act(rows)

    def by_edge(x, act):
        for condition, rows in ((x == 1, HALF + SHIFT), (x == 2, HALF - SHIFT), ((x == 0) | (x == 3), HALF)):

            @pl.when(condition)
            def _():
                act(rows)

    def send_fill(rows):
        for k in range(2):
            send(latest.at[:rows], fill.at[1 - k, :rows], first_r, at_x[k])

    def send_first(rows):
        for k in range(2):
            send_block(rows, BLOCK, me, first_r, k)

    def take_first(rows):
        wait(given_v.at[: BLOCK + rows], first_r)
        narrow_fill(0, right, rows)
        narrow_fill(1, left, rows)

    average(0)
    for c in range(2, len(READS) - 1):
        start_read(c)
    average(1)
    for copy in small:
        copy.wait()
    rows_r[z, y, core, me] = (weight_v[...] * gain_v[...]).astype(jnp.bfloat16)
    pl.semaphore_wait(barrier, jnp.where(lead, 6 + 2 * lax.rem(z, 2), 3))

    send_sums(0)
    by_core(send_fill)
    mine = rows_r.at[z, y, core, me]
    for k in range(3):
        send(mine, mine, x_r, at_x[k])

    @pl.when(lead)
    def _():
        tell(near, clear)

    @pl.when(lead & jnp.logical_not(even))
    def _():
        tell(above, clear)

    for c in range(2, len(READS) - 1):
        average(c)
    send_sums(1)

    wait_sums(0)
    narrow(0, BLOCK)
    by_core(send_first)
    narrow(BLOCK, EARLY)
    send_block(BLOCK, EARLY, me, pass_r.at[0], 0)
    send_block(BLOCK, EARLY, me, last_r, 1)
    wait_sums(1)
    narrow(EARLY, ROWS)

    def send_rest(edge):
        send_block(EARLY, edge, me, pass_r.at[0], 0)
        send_block(edge, ROWS, me, pass_r.at[1], 1)
        send_block(edge, ROWS, me, last_r, 0)
        send_block(EARLY, edge, me, last_r, 1)

    by_edge(me, send_rest)
    by_core(take_first)

    @pl.when(lead)
    def _():
        pl.semaphore_wait(clear, 5)
        tell(at_x, clear)

    @pl.when(lead & even)
    def _():
        tell(above, clear)

    @pl.when(jnp.logical_not(lead))
    def _():
        pl.semaphore_wait(clear, 1)

    wait(rows_r.at[z, y, core, : NX - 1], x_r)
    line = rows_r.at[z, y, core]
    send(line, line, y_r.at[0], at_y_up)
    send(line, line, y_r.at[0], at_y_down)
    wait(rows_r.at[z, :2, core], y_r.at[0])
    line = rows_r.at[z, y_down, core]
    send(line, line, y_r.at[1], at_y_up)
    wait(line, y_r.at[1])

    for step in range(NZ // 2):
        plane = rows_r.at[lax.rem(z + NZ - step, NZ), :, core]
        send(plane, plane, z_r.at[step], at_z_up)
        if step < NZ // 2 - 1:
            plane = rows_r.at[lax.rem(z + step, NZ), :, core]
            send(plane, plane, z_r.at[step], at_z_down)
            wait(rows_r.at[:2, :, core], z_r.at[step])
        else:
            wait(plane, z_r.at[step])

    def pass_right(edge):
        wait(block_of(BLOCK, edge, left), pass_r.at[0])
        send_block(0, edge, left, last_r, 0)

    def pass_left(edge):
        wait(block_of(edge, ROWS, right), pass_r.at[1])
        send_block(edge, ROWS, right, last_r, 1)

    by_edge(left, pass_right)
    by_edge(right, pass_left)

    side = rows_r.at[:, :, core]
    send(side, side, core_r, at_core)
    wait(side, core_r)

    def widen(i, carry):
        for j in range(NC):
            for x in range(NX):
                piece = rows_r[i // NY, lax.rem(i, NY), j, x].astype(jnp.float32)
                wide_r[i, 2 * j : 2 * j + 2, x * PART : (x + 1) * PART] = piece
        return carry

    lax.fori_loop(0, NZ * NY, widen, 0)

    def turn(i, carry):
        columns = pl.ds(pl.multiple_of(i * 128, 128), 128)
        tile = wide_r[:, :, columns].reshape(128, 128)
        router[columns, :] = tile.T.astype(jnp.bfloat16)
        return carry

    lax.fori_loop(0, D_MODEL // 128, turn, 0)

    def end(shift):
        wait(given_v.at[: (2 * ROWS - BLOCK + shift) // 2], last_r)

        def end_core(rows):
            blocks = 2 * (ROWS - BLOCK) + ROWS - shift + 2 * (BLOCK + rows)
            sums_and_router = 3 * BLOCKS // 2 + 3 * 2 + 3 * 8 + 7 * 32 + 256
            wait(given_v.at[: (blocks + sums_and_router) // 2], out_sem)

        by_core(end_core)

    @pl.when((me == 0) | (me == 3))
    def _():
        end(SHIFT)

    @pl.when((me == 1) | (me == 2))
    def _():
        end(-SHIFT)


def write(ready, scale, router, latest, ready_out, scale_out, router_out, latest_out, sem):
    pairs = (ready, ready_out), (latest, latest_out), (router, router_out), (scale, scale_out)
    copies = [pltpu.make_async_copy(src, dst, sem.at[i]) for i, (src, dst) in enumerate(pairs)]
    for copy in copies:
        copy.start()
    for copy in copies:
        copy.wait()


def shards(train_down, other_down, router_weight, router_gain):
    f32, bf16 = jnp.float32, jnp.bfloat16
    dma = pltpu.SemaphoreType.DMA
    shapes = (((ROWS, D_MODEL), bf16), ((2, ROWS // 2), f32), ((D_MODEL, 128), bf16), ((ROWS, PART), f32))
    given = (
        train_down.reshape(ROWS, PART),
        other_down.reshape(ROWS, PART),
        router_weight.T,
        router_gain.reshape(1, PART),
    )
    made = pl.pallas_call(
        kernel,
        out_shape=tuple(pltpu.VMEM(*k) for k in shapes),
        in_specs=[pl.BlockSpec(memory_space=pltpu.HBM)] * 4,
        out_specs=[pl.BlockSpec(memory_space=pltpu.VMEM)] * 4,
        scratch_shapes=[
            pltpu.VMEM((2 * ROWS, PART), f32),
            pltpu.VMEM((2, PART), f32),
            pltpu.VMEM((1, PART), f32),
            pltpu.VMEM((NX, BLOCKS, 1, BLOCK), f32),
            pltpu.VMEM((2, max(FILL), PART), f32),
            pltpu.VMEM((NZ, NY, NC, NX, 2, PART), bf16),
            pltpu.VMEM((NZ * NY, 2 * NC, D_MODEL), f32),
            pltpu.SemaphoreType.REGULAR,
            dma((len(READS) - 1,)), dma((2,)), dma, dma((2,)), dma, dma((2,)), dma((NZ // 2,)), dma, dma, dma((2,)), dma,
        ],
        compiler_params=pltpu.CompilerParams(
            collective_id=0, has_side_effects=True, vmem_limit_bytes=16 * 2**20
        ),
    )(*(pltpu.with_memory_space_constraint(k, pltpu.HBM) for k in given))
    ready, scale, router, latest = pl.pallas_call(
        write,
        out_shape=tuple(pltpu.HBM(*k) for k in shapes),
        in_specs=[pl.BlockSpec(memory_space=pltpu.VMEM)] * 4,
        out_specs=[pl.BlockSpec(memory_space=pltpu.HBM)] * 4,
        scratch_shapes=[dma((4,))],
        compiler_params=pltpu.CompilerParams(vmem_limit_bytes=2**20),
    )(*made)
    return ready.reshape(2, ROWS // 2, D_MODEL), scale, router, latest.reshape(2, ROWS // 2, PART)


def solution(mesh):
    return jax.shard_map(
        shards,
        mesh=mesh,
        in_specs=(P("bank", None, "zero"), P("bank", None, "zero"), P("zero", "bank"), P("zero")),
        out_specs=(P("bank", None, None), P("bank", None), P(), P("bank", None, "zero")),
        check_vma=False,
    )
```

```python
import jax
import jax.numpy as jnp
from jax import lax
from jax.experimental import pallas as pl
from jax.experimental.pallas import tpu as pltpu
from jax.sharding import PartitionSpec as P

MESH = pl.DeviceIdType.MESH
D_MODEL = 2048
ROWS = 1536
PART = 512
BLOCK = 128
BLOCKS = ROWS // BLOCK
FILL = (48, 64)
READS = (0, 128, 256, 768, 1536)
EARLY = 256
HALF = ROWS // 2
SHIFT = 32
NZ, NY, NC, NX = 8, 4, 2, 4


def kernel(
    train, other, weight, gain,
    ready, scale, router, latest,
    given_v, weight_v, gain_v, sums, fill, rows_r, wide_r,
    clear, in_sem, small_sem, out_sem, sum_r, x_r, y_r, z_r, core_r, first_r, pass_r, last_r,
):
    me = lax.axis_index("zero")
    bank = lax.axis_index("bank")
    z, y, core = bank // (NY * NC), lax.rem(bank // NC, NY), lax.rem(bank, NC)
    right, left, opposite = (lax.rem(me + k, NX) for k in (1, 3, 2))
    bank_of = lambda z, y, core: (z * NY + y) * NC + core
    z_up, z_down = lax.rem(z + 1, NZ), lax.rem(z + NZ - 1, NZ)
    y_up, y_down = lax.rem(y + 1, NY), lax.rem(y + NY - 1, NY)
    at_y_up, at_y_down = {"bank": bank_of(z, y_up, core)}, {"bank": bank_of(z, y_down, core)}
    at_z_up, at_z_down = {"bank": bank_of(z_up, y, core)}, {"bank": bank_of(z_down, y, core)}
    at_core = {"bank": bank_of(z, y, 1 - core)}
    at_x = [{"zero": right}, {"zero": left}, {"zero": opposite}]
    lead = me == 0
    even = lax.rem(z, 2) == 0
    near, above = (at_y_up, at_y_down, at_core), (at_z_up, at_z_down)
    barrier = pltpu.get_barrier_semaphore()

    def tell(peers, semaphore):
        for peer in peers:
            pl.semaphore_signal(semaphore, inc=1, device_id=peer, device_id_type=MESH)

    tell(at_x, barrier)

    @pl.when(lead)
    def _():
        tell(near, barrier)

    @pl.when(lead & even)
    def _():
        tell(above, barrier)

    def start_read(c):
        first, last = READS[c], READS[c + 1]
        for k, source in enumerate((train, other)):
            pltpu.make_async_copy(
                source.at[first:last], given_v.at[k * ROWS + first : k * ROWS + last], in_sem.at[c]
            ).start()

    def wait(size, semaphore):
        pltpu.make_async_copy(size, size, semaphore).wait()

    small = [
        pltpu.make_async_copy(weight, weight_v, small_sem.at[0]),
        pltpu.make_async_copy(gain, gain_v, small_sem.at[1]),
    ]
    for copy in small:
        copy.start()
    start_read(0)
    start_read(1)

    def send(src, dst, r, to):
        pltpu.make_async_remote_copy(
            src_ref=src, dst_ref=dst, send_sem=out_sem, recv_sem=r, device_id=to, device_id_type=MESH
        ).start()

    def average(c):
        wait(given_v.at[: 2 * (READS[c + 1] - READS[c])], in_sem.at[c])
        for b in range(READS[c] // BLOCK, READS[c + 1] // BLOCK):
            first, last = b * BLOCK, (b + 1) * BLOCK
            mixed = 0.5 * given_v[ROWS + first : ROWS + last, :] + 0.5 * given_v[first:last, :]
            latest[first:last, :] = mixed
            size = jnp.abs(mixed)
            lanes = sum(size[:, k * 128 : (k + 1) * 128] for k in range(1, PART // 128)) + size[:, :128]
            sums[me, b] = jnp.sum(lanes.T, axis=0, keepdims=True)

    def sums_of(x, group):
        first, last = ((0, EARLY), (EARLY, ROWS))[group]
        return sums.at[x, first // BLOCK : last // BLOCK]

    def send_sums(group):
        for k in (2, 0, 1):
            send(sums_of(me, group), sums_of(me, group), sum_r.at[group], at_x[k])

    def wait_sums(group):
        wait(sums_of(slice(0, NX - 1), group), sum_r.at[group])

    def mean(b):
        return ((sums[0, b] + sums[1, b]) + (sums[2, b] + sums[3, b])) / D_MODEL

    def factor(b):
        return jnp.broadcast_to(1.0 / mean(b), (BLOCK, BLOCK)).T

    def narrow(first, last):
        for b in range(first // BLOCK, last // BLOCK):
            rows = pl.ds(b * BLOCK, BLOCK)
            per = BLOCKS // 2
            scale[b // per : b // per + 1, (b % per) * BLOCK : (b % per + 1) * BLOCK] = mean(b)
            times = factor(b)
            for k in range(PART // 128):
                columns = pl.ds(pl.multiple_of(me * PART + k * 128, 128), 128)
                ready[rows, columns] = (latest[rows, k * 128 : (k + 1) * 128] * times).astype(jnp.bfloat16)

    def narrow_fill(side, x, rows):
        times = factor(0)[:rows]
        for k in range(PART // 128):
            columns = pl.ds(pl.multiple_of(x * PART + k * 128, 128), 128)
            ready[:rows, columns] = (fill[side, :rows, k * 128 : (k + 1) * 128] * times).astype(jnp.bfloat16)

    def block_of(first, last, x):
        return ready.at[pl.ds(first, last - first), pl.ds(pl.multiple_of(x * PART, PART), PART)]

    def send_block(first, last, x, r, k):
        block = block_of(first, last, x)
        send(block, block, r, at_x[k])

    def by_core(act):
        for i, rows in enumerate(FILL):

            @pl.when(core == i)
            def _():
                act(rows)

    def by_edge(x, act):
        for condition, rows in ((x == 1, HALF + SHIFT), (x == 2, HALF - SHIFT), ((x == 0) | (x == 3), HALF)):

            @pl.when(condition)
            def _():
                act(rows)

    def send_fill(rows):
        for k in range(2):
            send(latest.at[:rows], fill.at[1 - k, :rows], first_r, at_x[k])

    def send_first(rows):
        for k in range(2):
            send_block(rows, BLOCK, me, first_r, k)

    def take_first(rows):
        wait(given_v.at[: BLOCK + rows], first_r)
        narrow_fill(0, right, rows)
        narrow_fill(1, left, rows)

    average(0)
    average(1)
    for c in range(2, len(READS) - 1):
        start_read(c)
    for copy in small:
        copy.wait()
    rows_r[z, y, core, me] = (weight_v[...] * gain_v[...]).astype(jnp.bfloat16)
    pl.semaphore_wait(barrier, jnp.where(lead, 6 + 2 * lax.rem(z, 2), 3))

    send_sums(0)
    by_core(send_fill)
    mine = rows_r.at[z, y, core, me]
    for k in range(3):
        send(mine, mine, x_r, at_x[k])

    @pl.when(lead)
    def _():
        tell(near, clear)

    @pl.when(lead & jnp.logical_not(even))
    def _():
        tell(above, clear)

    for c in range(2, len(READS) - 1):
        average(c)
    send_sums(1)

    wait_sums(0)
    narrow(0, BLOCK)
    by_core(send_first)
    narrow(BLOCK, EARLY)
    send_block(BLOCK, EARLY, me, pass_r.at[0], 0)
    send_block(BLOCK, EARLY, me, last_r, 1)
    wait_sums(1)
    narrow(EARLY, ROWS)

    def send_rest(edge):
        send_block(EARLY, edge, me, pass_r.at[0], 0)
        send_block(edge, ROWS, me, pass_r.at[1], 1)
        send_block(edge, ROWS, me, last_r, 0)
        send_block(EARLY, edge, me, last_r, 1)

    by_edge(me, send_rest)
    by_core(take_first)

    @pl.when(lead)
    def _():
        pl.semaphore_wait(clear, 5)
        tell(at_x, clear)

    @pl.when(lead & even)
    def _():
        tell(above, clear)

    @pl.when(jnp.logical_not(lead))
    def _():
        pl.semaphore_wait(clear, 1)

    wait(rows_r.at[z, y, core, : NX - 1], x_r)
    line = rows_r.at[z, y, core]
    send(line, line, y_r.at[0], at_y_up)
    send(line, line, y_r.at[0], at_y_down)
    wait(rows_r.at[z, :2, core], y_r.at[0])
    line = rows_r.at[z, y_down, core]
    send(line, line, y_r.at[1], at_y_up)
    wait(line, y_r.at[1])

    for step in range(NZ // 2):
        plane = rows_r.at[lax.rem(z + NZ - step, NZ), :, core]
        send(plane, plane, z_r.at[step], at_z_up)
        if step < NZ // 2 - 1:
            plane = rows_r.at[lax.rem(z + step, NZ), :, core]
            send(plane, plane, z_r.at[step], at_z_down)
            wait(rows_r.at[:2, :, core], z_r.at[step])
        else:
            wait(plane, z_r.at[step])

    def pass_right(edge):
        wait(block_of(BLOCK, edge, left), pass_r.at[0])
        send_block(0, edge, left, last_r, 0)

    def pass_left(edge):
        wait(block_of(edge, ROWS, right), pass_r.at[1])
        send_block(edge, ROWS, right, last_r, 1)

    by_edge(left, pass_right)
    by_edge(right, pass_left)

    side = rows_r.at[:, :, core]
    send(side, side, core_r, at_core)
    wait(side, core_r)

    def widen(i, carry):
        for j in range(NC):
            for x in range(NX):
                piece = rows_r[i // NY, lax.rem(i, NY), j, x].astype(jnp.float32)
                wide_r[i, 2 * j : 2 * j + 2, x * PART : (x + 1) * PART] = piece
        return carry

    lax.fori_loop(0, NZ * NY, widen, 0)

    def turn(i, carry):
        columns = pl.ds(pl.multiple_of(i * 128, 128), 128)
        tile = wide_r[:, :, columns].reshape(128, 128)
        router[columns, :] = tile.T.astype(jnp.bfloat16)
        return carry

    lax.fori_loop(0, D_MODEL // 128, turn, 0)

    def end(shift):
        wait(given_v.at[: (2 * ROWS - BLOCK + shift) // 2], last_r)

        def end_core(rows):
            blocks = 2 * (ROWS - BLOCK) + ROWS - shift + 2 * (BLOCK + rows)
            sums_and_router = 3 * BLOCKS // 2 + 3 * 2 + 3 * 8 + 7 * 32 + 256
            wait(given_v.at[: (blocks + sums_and_router) // 2], out_sem)

        by_core(end_core)

    @pl.when((me == 0) | (me == 3))
    def _():
        end(SHIFT)

    @pl.when((me == 1) | (me == 2))
    def _():
        end(-SHIFT)


def write(ready, scale, router, latest, ready_out, scale_out, router_out, latest_out, sem):
    pairs = (ready, ready_out), (latest, latest_out), (router, router_out), (scale, scale_out)
    copies = [pltpu.make_async_copy(src, dst, sem.at[i]) for i, (src, dst) in enumerate(pairs)]
    for copy in copies:
        copy.start()
    for copy in copies:
        copy.wait()


def shards(train_down, other_down, router_weight, router_gain):
    f32, bf16 = jnp.float32, jnp.bfloat16
    dma = pltpu.SemaphoreType.DMA
    shapes = (((ROWS, D_MODEL), bf16), ((2, ROWS // 2), f32), ((D_MODEL, 128), bf16), ((ROWS, PART), f32))
    given = (
        train_down.reshape(ROWS, PART),
        other_down.reshape(ROWS, PART),
        router_weight.T,
        router_gain.reshape(1, PART),
    )
    made = pl.pallas_call(
        kernel,
        out_shape=tuple(pltpu.VMEM(*k) for k in shapes),
        in_specs=[pl.BlockSpec(memory_space=pltpu.HBM)] * 4,
        out_specs=[pl.BlockSpec(memory_space=pltpu.VMEM)] * 4,
        scratch_shapes=[
            pltpu.VMEM((2 * ROWS, PART), f32),
            pltpu.VMEM((2, PART), f32),
            pltpu.VMEM((1, PART), f32),
            pltpu.VMEM((NX, BLOCKS, 1, BLOCK), f32),
            pltpu.VMEM((2, max(FILL), PART), f32),
            pltpu.VMEM((NZ, NY, NC, NX, 2, PART), bf16),
            pltpu.VMEM((NZ * NY, 2 * NC, D_MODEL), f32),
            pltpu.SemaphoreType.REGULAR,
            dma((len(READS) - 1,)), dma((2,)), dma, dma((2,)), dma, dma((2,)), dma((NZ // 2,)), dma, dma, dma((2,)), dma,
        ],
        compiler_params=pltpu.CompilerParams(
            collective_id=0, has_side_effects=True, vmem_limit_bytes=16 * 2**20
        ),
    )(*(pltpu.with_memory_space_constraint(k, pltpu.HBM) for k in given))
    ready, scale, router, latest = pl.pallas_call(
        write,
        out_shape=tuple(pltpu.HBM(*k) for k in shapes),
        in_specs=[pl.BlockSpec(memory_space=pltpu.VMEM)] * 4,
        out_specs=[pl.BlockSpec(memory_space=pltpu.HBM)] * 4,
        scratch_shapes=[dma((4,))],
        compiler_params=pltpu.CompilerParams(vmem_limit_bytes=2**20),
    )(*made)
    return ready.reshape(2, ROWS // 2, D_MODEL), scale, router, latest.reshape(2, ROWS // 2, PART)


def solution(mesh):
    return jax.shard_map(
        shards,
        mesh=mesh,
        in_specs=(P("bank", None, "zero"), P("bank", None, "zero"), P("zero", "bank"), P("zero")),
        out_specs=(P("bank", None, None), P("bank", None), P(), P("bank", None, "zero")),
        check_vma=False,
    )
```

```python
import jax
import jax.numpy as jnp
from jax import lax
from jax.experimental import pallas as pl
from jax.experimental.pallas import tpu as pltpu
from jax.sharding import PartitionSpec as P

MESH = pl.DeviceIdType.MESH
D_MODEL = 2048
ROWS = 1536
PART = 512
BLOCK = 128
BLOCKS = ROWS // BLOCK
FILL = (48, 64)
READS = (0, 128, 384, 768, 1536)
EARLY = 384
HALF = ROWS // 2
SHIFT = 32
NZ, NY, NC, NX = 8, 4, 2, 4


def kernel(
    train, other, weight, gain,
    ready, scale, router, latest,
    given_v, weight_v, gain_v, sums, fill, rows_r, wide_r,
    clear, in_sem, small_sem, out_sem, sum_r, x_r, y_r, z_r, core_r, first_r, pass_r, last_r,
):
    me = lax.axis_index("zero")
    bank = lax.axis_index("bank")
    z, y, core = bank // (NY * NC), lax.rem(bank // NC, NY), lax.rem(bank, NC)
    right, left, opposite = (lax.rem(me + k, NX) for k in (1, 3, 2))
    bank_of = lambda z, y, core: (z * NY + y) * NC + core
    z_up, z_down = lax.rem(z + 1, NZ), lax.rem(z + NZ - 1, NZ)
    y_up, y_down = lax.rem(y + 1, NY), lax.rem(y + NY - 1, NY)
    at_y_up, at_y_down = {"bank": bank_of(z, y_up, core)}, {"bank": bank_of(z, y_down, core)}
    at_z_up, at_z_down = {"bank": bank_of(z_up, y, core)}, {"bank": bank_of(z_down, y, core)}
    at_core = {"bank": bank_of(z, y, 1 - core)}
    at_x = [{"zero": right}, {"zero": left}, {"zero": opposite}]
    lead = me == 0
    even = lax.rem(z, 2) == 0
    near, above = (at_y_up, at_y_down, at_core), (at_z_up, at_z_down)
    barrier = pltpu.get_barrier_semaphore()

    def tell(peers, semaphore):
        for peer in peers:
            pl.semaphore_signal(semaphore, inc=1, device_id=peer, device_id_type=MESH)

    tell(at_x, barrier)

    @pl.when(lead)
    def _():
        tell(near, barrier)

    @pl.when(lead & even)
    def _():
        tell(above, barrier)

    def start_read(c):
        first, last = READS[c], READS[c + 1]
        for k, source in enumerate((train, other)):
            pltpu.make_async_copy(
                source.at[first:last], given_v.at[k * ROWS + first : k * ROWS + last], in_sem.at[c]
            ).start()

    def wait(size, semaphore):
        pltpu.make_async_copy(size, size, semaphore).wait()

    small = [
        pltpu.make_async_copy(weight, weight_v, small_sem.at[0]),
        pltpu.make_async_copy(gain, gain_v, small_sem.at[1]),
    ]
    for copy in small:
        copy.start()
    start_read(0)
    start_read(1)

    def send(src, dst, r, to):
        pltpu.make_async_remote_copy(
            src_ref=src, dst_ref=dst, send_sem=out_sem, recv_sem=r, device_id=to, device_id_type=MESH
        ).start()

    def average(c):
        wait(given_v.at[: 2 * (READS[c + 1] - READS[c])], in_sem.at[c])
        for b in range(READS[c] // BLOCK, READS[c + 1] // BLOCK):
            first, last = b * BLOCK, (b + 1) * BLOCK
            mixed = 0.5 * given_v[ROWS + first : ROWS + last, :] + 0.5 * given_v[first:last, :]
            latest[first:last, :] = mixed
            size = jnp.abs(mixed)
            lanes = sum(size[:, k * 128 : (k + 1) * 128] for k in range(1, PART // 128)) + size[:, :128]
            sums[me, b] = jnp.sum(lanes.T, axis=0, keepdims=True)

    def sums_of(x, group):
        first, last = ((0, EARLY), (EARLY, ROWS))[group]
        return sums.at[x, first // BLOCK : last // BLOCK]

    def send_sums(group):
        for k in (2, 0, 1):
            send(sums_of(me, group), sums_of(me, group), sum_r.at[group], at_x[k])

    def wait_sums(group):
        wait(sums_of(slice(0, NX - 1), group), sum_r.at[group])

    def mean(b):
        return ((sums[0, b] + sums[1, b]) + (sums[2, b] + sums[3, b])) / D_MODEL

    def factor(b):
        return jnp.broadcast_to(1.0 / mean(b), (BLOCK, BLOCK)).T

    def narrow(first, last):
        for b in range(first // BLOCK, last // BLOCK):
            rows = pl.ds(b * BLOCK, BLOCK)
            per = BLOCKS // 2
            scale[b // per : b // per + 1, (b % per) * BLOCK : (b % per + 1) * BLOCK] = mean(b)
            times = factor(b)
            for k in range(PART // 128):
                columns = pl.ds(pl.multiple_of(me * PART + k * 128, 128), 128)
                ready[rows, columns] = (latest[rows, k * 128 : (k + 1) * 128] * times).astype(jnp.bfloat16)

    def narrow_fill(side, x, rows):
        times = factor(0)[:rows]
        for k in range(PART // 128):
            columns = pl.ds(pl.multiple_of(x * PART + k * 128, 128), 128)
            ready[:rows, columns] = (fill[side, :rows, k * 128 : (k + 1) * 128] * times).astype(jnp.bfloat16)

    def block_of(first, last, x):
        return ready.at[pl.ds(first, last - first), pl.ds(pl.multiple_of(x * PART, PART), PART)]

    def send_block(first, last, x, r, k):
        block = block_of(first, last, x)
        send(block, block, r, at_x[k])

    def by_core(act):
        for i, rows in enumerate(FILL):

            @pl.when(core == i)
            def _():
                act(rows)

    def by_edge(x, act):
        for condition, rows in ((x == 1, HALF + SHIFT), (x == 2, HALF - SHIFT), ((x == 0) | (x == 3), HALF)):

            @pl.when(condition)
            def _():
                act(rows)

    def send_fill(rows):
        for k in range(2):
            send(latest.at[:rows], fill.at[1 - k, :rows], first_r, at_x[k])

    def send_first(rows):
        for k in range(2):
            send_block(rows, BLOCK, me, first_r, k)

    def take_first(rows):
        wait(given_v.at[: BLOCK + rows], first_r)
        narrow_fill(0, right, rows)
        narrow_fill(1, left, rows)

    average(0)
    average(1)
    for c in range(2, len(READS) - 1):
        start_read(c)
    for copy in small:
        copy.wait()
    rows_r[z, y, core, me] = (weight_v[...] * gain_v[...]).astype(jnp.bfloat16)
    pl.semaphore_wait(barrier, jnp.where(lead, 6 + 2 * lax.rem(z, 2), 3))

    send_sums(0)
    by_core(send_fill)
    mine = rows_r.at[z, y, core, me]
    for k in range(3):
        send(mine, mine, x_r, at_x[k])

    @pl.when(lead)
    def _():
        tell(near, clear)

    @pl.when(lead & jnp.logical_not(even))
    def _():
        tell(above, clear)

    for c in range(2, len(READS) - 1):
        average(c)
    send_sums(1)

    wait_sums(0)
    narrow(0, BLOCK)
    by_core(send_first)
    narrow(BLOCK, EARLY)
    send_block(BLOCK, EARLY, me, pass_r.at[0], 0)
    send_block(BLOCK, EARLY, me, last_r, 1)
    wait_sums(1)
    narrow(EARLY, ROWS)

    def send_rest(edge):
        send_block(EARLY, edge, me, pass_r.at[0], 0)
        send_block(edge, ROWS, me, pass_r.at[1], 1)
        send_block(edge, ROWS, me, last_r, 0)
        send_block(EARLY, edge, me, last_r, 1)

    by_edge(me, send_rest)
    by_core(take_first)

    @pl.when(lead)
    def _():
        pl.semaphore_wait(clear, 5)
        tell(at_x, clear)

    @pl.when(lead & even)
    def _():
        tell(above, clear)

    @pl.when(jnp.logical_not(lead))
    def _():
        pl.semaphore_wait(clear, 1)

    wait(rows_r.at[z, y, core, : NX - 1], x_r)
    line = rows_r.at[z, y, core]
    send(line, line, y_r.at[0], at_y_up)
    send(line, line, y_r.at[0], at_y_down)
    wait(rows_r.at[z, :2, core], y_r.at[0])
    line = rows_r.at[z, y_down, core]
    send(line, line, y_r.at[1], at_y_up)
    wait(line, y_r.at[1])

    for step in range(NZ // 2):
        plane = rows_r.at[lax.rem(z + NZ - step, NZ), :, core]
        send(plane, plane, z_r.at[step], at_z_up)
        if step < NZ // 2 - 1:
            plane = rows_r.at[lax.rem(z + step, NZ), :, core]
            send(plane, plane, z_r.at[step], at_z_down)
            wait(rows_r.at[:2, :, core], z_r.at[step])
        else:
            wait(plane, z_r.at[step])

    def pass_right(edge):
        wait(block_of(BLOCK, edge, left), pass_r.at[0])
        send_block(0, edge, left, last_r, 0)

    def pass_left(edge):
        wait(block_of(edge, ROWS, right), pass_r.at[1])
        send_block(edge, ROWS, right, last_r, 1)

    by_edge(left, pass_right)
    by_edge(right, pass_left)

    side = rows_r.at[:, :, core]
    send(side, side, core_r, at_core)
    wait(side, core_r)

    def widen(i, carry):
        for j in range(NC):
            for x in range(NX):
                piece = rows_r[i // NY, lax.rem(i, NY), j, x].astype(jnp.float32)
                wide_r[i, 2 * j : 2 * j + 2, x * PART : (x + 1) * PART] = piece
        return carry

    lax.fori_loop(0, NZ * NY, widen, 0)

    def turn(i, carry):
        columns = pl.ds(pl.multiple_of(i * 128, 128), 128)
        tile = wide_r[:, :, columns].reshape(128, 128)
        router[columns, :] = tile.T.astype(jnp.bfloat16)
        return carry

    lax.fori_loop(0, D_MODEL // 128, turn, 0)

    def end(shift):
        wait(given_v.at[: (2 * ROWS - BLOCK + shift) // 2], last_r)

        def end_core(rows):
            blocks = 2 * (ROWS - BLOCK) + ROWS - shift + 2 * (BLOCK + rows)
            sums_and_router = 3 * BLOCKS // 2 + 3 * 2 + 3 * 8 + 7 * 32 + 256
            wait(given_v.at[: (blocks + sums_and_router) // 2], out_sem)

        by_core(end_core)

    @pl.when((me == 0) | (me == 3))
    def _():
        end(SHIFT)

    @pl.when((me == 1) | (me == 2))
    def _():
        end(-SHIFT)


def write(ready, scale, router, latest, ready_out, scale_out, router_out, latest_out, sem):
    pairs = (ready, ready_out), (latest, latest_out), (router, router_out), (scale, scale_out)
    copies = [pltpu.make_async_copy(src, dst, sem.at[i]) for i, (src, dst) in enumerate(pairs)]
    for copy in copies:
        copy.start()
    for copy in copies:
        copy.wait()


def shards(train_down, other_down, router_weight, router_gain):
    f32, bf16 = jnp.float32, jnp.bfloat16
    dma = pltpu.SemaphoreType.DMA
    shapes = (((ROWS, D_MODEL), bf16), ((2, ROWS // 2), f32), ((D_MODEL, 128), bf16), ((ROWS, PART), f32))
    given = (
        train_down.reshape(ROWS, PART),
        other_down.reshape(ROWS, PART),
        router_weight.T,
        router_gain.reshape(1, PART),
    )
    made = pl.pallas_call(
        kernel,
        out_shape=tuple(pltpu.VMEM(*k) for k in shapes),
        in_specs=[pl.BlockSpec(memory_space=pltpu.HBM)] * 4,
        out_specs=[pl.BlockSpec(memory_space=pltpu.VMEM)] * 4,
        scratch_shapes=[
            pltpu.VMEM((2 * ROWS, PART), f32),
            pltpu.VMEM((2, PART), f32),
            pltpu.VMEM((1, PART), f32),
            pltpu.VMEM((NX, BLOCKS, 1, BLOCK), f32),
            pltpu.VMEM((2, max(FILL), PART), f32),
            pltpu.VMEM((NZ, NY, NC, NX, 2, PART), bf16),
            pltpu.VMEM((NZ * NY, 2 * NC, D_MODEL), f32),
            pltpu.SemaphoreType.REGULAR,
            dma((len(READS) - 1,)), dma((2,)), dma, dma((2,)), dma, dma((2,)), dma((NZ // 2,)), dma, dma, dma((2,)), dma,
        ],
        compiler_params=pltpu.CompilerParams(
            collective_id=0, has_side_effects=True, vmem_limit_bytes=16 * 2**20
        ),
    )(*(pltpu.with_memory_space_constraint(k, pltpu.HBM) for k in given))
    ready, scale, router, latest = pl.pallas_call(
        write,
        out_shape=tuple(pltpu.HBM(*k) for k in shapes),
        in_specs=[pl.BlockSpec(memory_space=pltpu.VMEM)] * 4,
        out_specs=[pl.BlockSpec(memory_space=pltpu.HBM)] * 4,
        scratch_shapes=[dma((4,))],
        compiler_params=pltpu.CompilerParams(vmem_limit_bytes=2**20),
    )(*made)
    return ready.reshape(2, ROWS // 2, D_MODEL), scale, router, latest.reshape(2, ROWS // 2, PART)


def solution(mesh):
    return jax.shard_map(
        shards,
        mesh=mesh,
        in_specs=(P("bank", None, "zero"), P("bank", None, "zero"), P("zero", "bank"), P("zero")),
        out_specs=(P("bank", None, None), P("bank", None), P(), P("bank", None, "zero")),
        check_vma=False,
    )
```
